32 devices in a mesh: row: 4 (over z), col: 8 (over y, x, core).
Axes of the slice: x: 2, y: 2, z: 4, core: 2. Of those that a mesh axis runs over, the one named last changes fastest.
Arguments:
- rhs: float32 [64, 131072], P(None, ('row', 'col')), may hold values from -6 to 6
- pivots: int32 [4096], replicated, may hold values from 0 to 131071, as said below
- factor: float32 [4096, 4, 8, 128], P('row', None, 'col'), as said below
- diag_inv: float32 [8, 512, 512], P('row'), as said below
Outputs:
- solution: float32 [64, 4, 8, 128], P(None, None, 'col')
The draws below stay inside these ranges and needn't reach their ends.
Inputs may be any that keep to these rules, and one draw needn't show every extreme that they name: `pivots`: distinct column numbers, the first 4096 entries of a permutation of 0 .. 131071. `factor`: entry (row i, column q) is zero where q >= 512 * (i // 512). `diag_inv`: each block is unit lower triangular.
All inputs are finite; a program needn't handle non-finite values.
Results may differ from the reference program's by a relative error of at most 0.0001.
Values sent between devices are 32-bit elements; how exact they have to be, the bound alone decides.
A program may use at most 64 MiB of HBM per device.

```python
import math
import jax
import jax.numpy as jnp
from jax import lax

N = 131072
BLK = 512
CB = 128
NRHS = 64
NB = 8
N_COL = 8


def draw_pivots(key, part):
    order = jax.random.permutation(jax.random.fold_in(key, 11), N)
    return order[:NB * BLK].astype(jnp.int32)


def draw_factor(key, part):
    width = NB * BLK
    rounds = NB * (BLK // CB) // N_COL
    shape = (width, rounds, N_COL, CB)
    row_block = lax.broadcasted_iota(jnp.int32, shape, 0) // BLK
    column = (lax.broadcasted_iota(jnp.int32, shape, 1) * N_COL + lax.broadcasted_iota(jnp.int32, shape, 2)) * CB + lax.broadcasted_iota(jnp.int32, shape, 3)
    col_block = column // BLK
    subkey = jax.random.fold_in(key, 23)
    values = jax.random.normal(subkey, shape, jnp.float32)
    values = values * (0.6 / math.sqrt(width))
    return jnp.where(col_block < row_block, values, 0.0).astype(jnp.float32)


def draw_diag_inv(key, part):
    shape = (NB, BLK, BLK)
    inner = lax.broadcasted_iota(jnp.int32, shape, 1)
    outer = lax.broadcasted_iota(jnp.int32, shape, 2)
    subkey = jax.random.fold_in(key, 37)
    values = jax.random.normal(subkey, shape, jnp.float32)
    values = values * (0.5 / math.sqrt(BLK))
    lower_part = jnp.where(outer < inner, values, 0.0)
    return (lower_part + jnp.where(outer == inner, 1.0, 0.0)).astype(jnp.float32)


def shard_levels(key, shape, cuts, smallest, largest):
    def one(axis_at, shards_of):
        draws = jax.random.uniform(jax.random.fold_in(jax.random.fold_in(key, 6), axis_at), (shards_of,), jnp.float32, smallest / len(cuts), largest / len(cuts))
        return jnp.repeat(jnp.exp(draws), shape[axis_at] // shards_of).reshape((-1,) + (1,) * (len(shape) - axis_at - 1))

    loudness = one(*cuts[0])
    for cut in cuts[1:]:
        loudness = loudness * one(*cut)
    return loudness


def gaussian(own_key, dims, scale, bound, cuts=(), dtype=jnp.bfloat16):
    loudness = shard_levels(own_key, dims, cuts, -0.22, 0.18) if cuts else 1.0
    drawn = jax.random.normal(own_key, dims, jnp.float32) * scale * loudness
    return jnp.minimum(jnp.maximum(drawn, -bound), bound).astype(dtype)


def setup_inputs(seed: int = 0) -> dict:
    key_list = jax.random.split(jax.random.key(seed), 5)
    rhs = gaussian(key_list[0], (NRHS, N), 1.0, 6.0, ((1, 32),), jnp.float32)
    pivots = draw_pivots(jax.random.fold_in(key_list[4], 71), 0)
    factor = draw_factor(jax.random.fold_in(key_list[4], 71), 0)
    diag_inv = draw_diag_inv(jax.random.fold_in(key_list[4], 71), 0)
    return dict(rhs=rhs, pivots=pivots, factor=factor, diag_inv=diag_inv)


def reference(rhs, pivots, factor, diag_inv):
    width = NB * BLK
    permuted = jnp.take(rhs, pivots, axis=1)
    full_lower = factor.reshape(width, width)

    def advance(number, solved):
        offset = (number * BLK).astype(jnp.int32)
        block_rows = lax.dynamic_slice_in_dim(full_lower, offset, BLK, 0)
        summed = lax.dot_general(solved, block_rows, (((1,), (1,)), ((), ())), precision=lax.Precision.HIGHEST, preferred_element_type=jnp.float32)
        own_rhs = lax.dynamic_slice_in_dim(permuted, offset, BLK, 1)
        block_inv = lax.dynamic_index_in_dim(diag_inv, number.astype(jnp.int32), 0, keepdims=False)
        fresh = lax.dot_general(own_rhs - summed, block_inv, (((1,), (1,)), ((), ())), precision=lax.Precision.HIGHEST, preferred_element_type=jnp.float32)
        return lax.dynamic_update_slice_in_dim(solved, fresh, offset, 1)

    solved = lax.fori_loop(jnp.int32(0), jnp.int32(NB), advance, jnp.zeros((NRHS, width), jnp.float32))
    return solved.reshape(NRHS, NB * (BLK // CB) // N_COL, N_COL, CB)
```

```python
import functools

import jax
import jax.numpy as jnp
from jax import lax
from jax.experimental import pallas as pl
from jax.experimental.pallas import tpu as pltpu
from jax.sharding import PartitionSpec as P


def broadcast(shard, axis, root):
    mine = lax.axis_index(axis) == root
    return lax.psum(jnp.where(mine, shard, jnp.zeros_like(shard)), axis)


def apply_inverse(values, block_inv):
    return lax.dot_general(
        values,
        block_inv,
        (((1,), (1,)), ((), ())),
        precision=lax.Precision.HIGHEST,
        preferred_element_type=jnp.float32,
    )


def per_device_general(rhs, pivots, factor, diag_inv):
    my_row = lax.axis_index("row")
    my_col = lax.axis_index("col")
    col_count = lax.axis_size("col")
    rhs_count = rhs.shape[0]
    slab_rows = factor.shape[0]
    rounds = factor.shape[1]
    piece_len = factor.shape[3]
    block_len = diag_inv.shape[1]
    pieces = block_len // piece_len
    blocks_here = slab_rows // block_len
    total_blocks = blocks_here * lax.axis_size("row")
    first_column = (my_row * col_count + my_col) * rhs.shape[1]
    source_len = rhs.shape[1]
    located = pivots - first_column
    inside = (located >= 0) & (located < source_len)
    taken = jnp.take(rhs, jnp.clip(located, 0, source_len - 1), axis=1)
    taken = jnp.where(inside[None, :], taken, 0.0)
    permuted = lax.psum_scatter(
        jnp.transpose(
            taken.reshape(rhs_count, blocks_here * lax.axis_size("row"), block_len), (1, 0, 2)
        ),
        "row",
        scatter_dimension=0,
        tiled=True,
    )
    permuted = lax.psum(permuted, "col")
    factor_rows = factor.reshape(slab_rows, rounds * piece_len)

    def advance(number, solved):
        owner_row = number // blocks_here
        local_block = number % blocks_here
        block_rows = lax.dynamic_slice_in_dim(factor_rows, local_block * block_len, block_len, 0)
        partial_value = lax.dot_general(
            solved.reshape(rhs_count, rounds * piece_len),
            block_rows,
            (((1,), (1,)), ((), ())),
            precision=lax.Precision.HIGHEST,
            preferred_element_type=jnp.float32,
        )
        own_rhs = lax.dynamic_index_in_dim(permuted, local_block, 0, keepdims=False)
        block_inv = lax.dynamic_index_in_dim(diag_inv, local_block, 0, keepdims=False)
        summed = lax.psum(partial_value, "col")
        fresh = apply_inverse(own_rhs - summed, block_inv)
        fresh = broadcast(fresh, "row", owner_row)
        first_piece = number * pieces
        offset_piece = (my_col - first_piece) % col_count
        owns = offset_piece < pieces
        which = jnp.clip(offset_piece, 0, pieces - 1)
        local_round = jnp.clip((first_piece + offset_piece) // col_count, 0, rounds - 1)
        piece = lax.dynamic_slice_in_dim(fresh, which * piece_len, piece_len, 1)
        updated = lax.dynamic_update_index_in_dim(solved, piece[:, None, :], local_round, 1)
        return jnp.where(owns, updated, solved)

    start_state = jnp.zeros((rhs_count, rounds, 1, piece_len), jnp.float32)
    return lax.fori_loop(0, total_blocks, advance, start_state)


MESH = pl.DeviceIdType.MESH
HIGH = lax.Precision.HIGHEST


def mul(a, b):
    return jnp.dot(a, b, precision=HIGH, preferred_element_type=jnp.float32)


def mul_t(a, b):
    return lax.dot_general(
        a, b, (((1,), (1,)), ((), ())), precision=HIGH, preferred_element_type=jnp.float32
    )


def solve_kernel(
    rows,
    cols,
    g_ref,
    fac_ref,
    diag_ref,
    out_ref,
    lf,
    dg,
    s0,
    a1,
    b1,
    ab2,
    zbuf,
    brow,
    l10,
    m,
    w,
    part,
    pbuf,
    ybuf,
    local_sem,
    ssend,
    srecv,
    zsend,
    zrecv,
    gsend,
    grecv,
    lsend,
    lrecv,
    psend,
    precv,
    ysend,
    yrecv,
):
    r = lax.axis_index("row")
    c = lax.axis_index("col")
    core, x, y = c % 2, (c // 2) % 2, c // 4
    half = rows // 2
    blk = dg.shape[1]
    plen = lf.shape[2]
    slots = cols // 2
    to_core = c + 1 - 2 * core
    to_x = c + 2 * (1 - 2 * x)
    to_y = c + 4 * (1 - 2 * y)

    fetch = [
        pltpu.make_async_copy(fac_ref.at[:, k, 0, :], lf.at[k], local_sem.at[k])
        for k in range(rows)
    ]
    for copy in fetch:
        copy.start()
    fetch_d = pltpu.make_async_copy(diag_ref, dg, local_sem.at[rows])
    fetch_d.start()

    barrier = pltpu.get_barrier_semaphore()
    for d in range(1, cols):
        pl.semaphore_signal(barrier, inc=1, device_id=(r, (c + d) % cols), device_id_type=MESH)
    for d in range(1, rows):
        pl.semaphore_signal(barrier, inc=1, device_id=((r + d) % rows, c), device_id_type=MESH)
    pl.semaphore_wait(barrier, cols + rows - 2)

    def remote(src, dst, send, recv, row, col):
        return pltpu.make_async_remote_copy(
            src_ref=src,
            dst_ref=dst,
            send_sem=send,
            recv_sem=recv,
            device_id=(row, col),
            device_id_type=MESH,
        )

    c0 = remote(g_ref.at[1 - core], s0, ssend.at[0], srecv.at[0], r, to_core)
    c0.start()

    mine = c % slots
    xflip = mine + 2 * (1 - 2 * x)
    cflip = mine + 1 - 2 * core
    bflip = xflip + 1 - 2 * core
    ly = remote(l10.at[mine], l10.at[mine], lsend.at[0], lrecv.at[0], r, to_y)
    lx = remote(l10.at[mine], l10.at[mine], lsend.at[1], lrecv.at[1], r, to_x)
    lc = remote(l10.at[mine], l10.at[mine], lsend.at[2], lrecv.at[2], r, to_core)
    lb = remote(l10.at[xflip], l10.at[xflip], lsend.at[3], lrecv.at[3], r, to_core)
    for copy in fetch:
        copy.wait()

    @pl.when(y == 0)
    def _():
        l10[mine] = lf[r, blk:, :]
        ly.start()
        lx.start()
        lc.start()

    c0.wait()
    s0[...] += g_ref[core]
    cxa = remote(s0.at[1 - x, :, pl.ds(0, half)], a1, ssend.at[1], srecv.at[1], r, to_x)
    cyb = remote(s0.at[:, 1 - y, pl.ds(half, half)], b1, ssend.at[2], srecv.at[2], r, to_y)
    cxa.start()
    cyb.start()

    @pl.when(y == 1)
    def _():
        ly.wait_recv()
        lx.start()
        lc.start()

    cxa.wait()
    a1[...] += s0[x, :, pl.ds(0, half)]
    cya = remote(a1.at[1 - y], ab2.at[pl.ds(0, half)], ssend.at[3], srecv.at[3], r, to_y)
    cya.start()
    cyb.wait()
    b1[...] += s0[:, y, pl.ds(half, half)]
    cxb = remote(b1.at[1 - x], ab2.at[pl.ds(half, half)], ssend.at[4], srecv.at[4], r, to_x)
    cxb.start()

    fetch_d.wait()
    lower = jnp.concatenate([lf[k, :blk, :] for k in range(rows - 1)], axis=1)
    m[:blk, :] = mul(dg[0], lower)

    cya.wait()
    cxb.wait()
    ab2[pl.ds(0, half)] += a1[y]
    ab2[pl.ds(half, half)] += b1[x]
    zc = [None]
    for d in range(1, rows):
        to = (r + d) % rows
        copy = remote(ab2.at[to], zbuf.at[d], zsend.at[d], zrecv.at[d], to, c)
        copy.start()
        zc.append(copy)

    lx.wait_recv()
    lb.start()

    for d in range(1, rows):
        zc[d].wait_recv()
    piece = ab2[r]
    for d in range(1, rows):
        piece = piece + zbuf[d]
    brow[c] = piece
    gc = [None]
    for d in range(1, cols):
        copy = remote(
            brow.at[c], brow.at[c], gsend.at[d], grecv.at[d], r, (c + d) % cols
        )
        copy.start()
        gc.append(copy)

    lc.wait_recv()
    lb.wait_recv()
    l10v = jnp.concatenate([l10[t] for t in range(slots)], axis=1)
    below = jnp.concatenate([lf[k, blk:, :] for k in range(rows - 1)], axis=1)
    m[blk:, :] = mul(dg[1], below - mul(l10v, m[:blk, :]))

    @pl.when(c < slots)
    def _():
        w[:, :blk] = dg[0, pl.ds(pl.multiple_of(mine * plen, plen), plen), :]
        w[:, blk:] = jnp.zeros((plen, blk), jnp.float32)

    @pl.when(c >= slots)
    def _():
        u = dg[1, pl.ds(pl.multiple_of(mine * plen, plen), plen), :]
        w[:, blk:] = u
        l10w = jnp.concatenate([l10[t] for t in range(slots)], axis=1)
        w[:, :blk] = -mul(mul(u, l10w), dg[0])

    for d in range(1, cols):
        gc[d].wait_recv()
    b = jnp.concatenate([brow[s] for s in range(cols)], axis=1)
    own = mul_t(b, w[...])

    pc = [
        remote(
            part.at[(c + d) % cols], pbuf.at[d], psend.at[d], precv.at[d], r, (c + d) % cols
        )
        for d in range(1, cols)
    ]
    for k in range(rows):
        yc = [
            remote(
                ybuf.at[k],
                ybuf.at[k],
                ysend.at[d],
                yrecv.at[k],
                (k + d) % rows,
                c,
            )
            for d in range(1, rows)
        ]

        @pl.when(r == k)
        def _():
            if k == 0:
                ybuf[k] = own
            else:
                total = part[c]
                for copy in pc:
                    copy.wait_recv()
                for d in range(1, cols):
                    total = total + pbuf[d]
                ybuf[k] = own - total
            for copy in yc:
                copy.start()

        @pl.when(r != k)
        def _():
            yc[0].wait_recv()

        if k < rows - 1:

            @pl.when(r > k)
            def _():
                add = mul_t(ybuf[k], m[:, k * plen : (k + 1) * plen])
                for p in range(cols):
                    now = add[:, p * plen : (p + 1) * plen]
                    part[p] = now if k == 0 else part[p] + now

            @pl.when(r == k + 1)
            def _():
                for copy in pc:
                    copy.start()

    out_ref[...] = ybuf[...]

    for d in range(1, rows):
        zc[d].wait_send()

    @pl.when(y == 0)
    def _():
        ly.wait_send()

    lx.wait_send()
    lc.wait_send()
    lb.wait_send()
    for d in range(1, cols):
        gc[d].wait_send()

    @pl.when(r > 0)
    def _():
        for copy in pc:
            copy.wait_send()

    for d in range(1, rows):
        remote(
            ybuf.at[r], ybuf.at[r], ysend.at[d], yrecv.at[r], (r + d) % rows, c
        ).wait_send()


def per_device_fast(rows, cols, rhs, pivots, factor, diag_inv):
    my_row = lax.axis_index("row")
    my_col = lax.axis_index("col")
    nrhs, source_len = rhs.shape
    plen = factor.shape[3]
    blk = diag_inv.shape[1]
    slab = factor.shape[0]
    half = rows // 2
    slots = cols // 2
    first_column = (my_row * cols + my_col) * source_len
    order = pivots.reshape(rows, 2, 2, 2, plen).transpose(3, 2, 1, 0, 4).reshape(-1)
    located = order - first_column
    inside = (located >= 0) & (located < source_len)
    taken = jnp.take(rhs, jnp.clip(located, 0, source_len - 1), axis=1)
    taken = jnp.where(inside[None, :], taken, 0.0)
    g = taken.reshape(nrhs, 2, 2, 2, rows, plen).transpose(1, 2, 3, 4, 0, 5)
    f32 = jnp.float32
    dma = pltpu.SemaphoreType.DMA
    solved = pl.pallas_call(
        functools.partial(solve_kernel, rows, cols),
        out_shape=jax.ShapeDtypeStruct((rows, nrhs, plen), f32),
        in_specs=[
            pl.BlockSpec(memory_space=pltpu.VMEM),
            pl.BlockSpec(memory_space=pl.ANY),
            pl.BlockSpec(memory_space=pl.ANY),
        ],
        out_specs=pl.BlockSpec(memory_space=pltpu.VMEM),
        scratch_shapes=[
            pltpu.VMEM((rows, slab, plen), f32),
            pltpu.VMEM((2, blk, blk), f32),
            pltpu.VMEM((2, 2, rows, nrhs, plen), f32),
            pltpu.VMEM((2, half, nrhs, plen), f32),
            pltpu.VMEM((2, half, nrhs, plen), f32),
            pltpu.VMEM((rows, nrhs, plen), f32),
            pltpu.VMEM((rows, nrhs, plen), f32),
            pltpu.VMEM((cols, nrhs, plen), f32),
            pltpu.VMEM((slots, blk, plen), f32),
            pltpu.VMEM((slab, (rows - 1) * plen), f32),
            pltpu.VMEM((plen, slab), f32),
            pltpu.VMEM((cols, nrhs, plen), f32),
            pltpu.VMEM((cols, nrhs, plen), f32),
            pltpu.VMEM((rows, nrhs, plen), f32),
            dma((rows + 1,)),
            dma((5,)),
            dma((5,)),
            dma((rows,)),
            dma((rows,)),
            dma((cols,)),
            dma((cols,)),
            dma((4,)),
            dma((4,)),
            dma((cols,)),
            dma((cols,)),
            dma((rows,)),
            dma((rows,)),
        ],
        compiler_params=pltpu.CompilerParams(collective_id=0, has_side_effects=True),
    )(g, factor, diag_inv)
    return jnp.transpose(solved, (1, 0, 2))[:, :, None, :]


def per_device(rhs, pivots, factor, diag_inv):
    rows = lax.axis_size("row")
    cols = lax.axis_size("col")
    slab, rounds, _, plen = factor.shape
    blk = diag_inv.shape[1]
    if cols == 8 and slab == 2 * blk == cols * plen and rounds == rows and rows % 2 == 0:
        return per_device_fast(rows, cols, rhs, pivots, factor, diag_inv)
    return per_device_general(rhs, pivots, factor, diag_inv)


def solution(mesh):
    return jax.shard_map(
        per_device,
        mesh=mesh,
        in_specs=(P(None, ("row", "col")), P(), P("row", None, "col", None), P("row", None, None)),
        out_specs=P(None, None, "col", None),
        check_vma=False,
    )
```

```python
import functools

import jax
import jax.numpy as jnp
from jax import lax
from jax.experimental import pallas as pl
from jax.experimental.pallas import tpu as pltpu
from jax.sharding import PartitionSpec as P


def broadcast(shard, axis, root):
    mine = lax.axis_index(axis) == root
    return lax.psum(jnp.where(mine, shard, jnp.zeros_like(shard)), axis)


def apply_inverse(values, block_inv):
    return lax.dot_general(
        values,
        block_inv,
        (((1,), (1,)), ((), ())),
        precision=lax.Precision.HIGHEST,
        preferred_element_type=jnp.float32,
    )


def per_device_general(rhs, pivots, factor, diag_inv):
    my_row = lax.axis_index("row")
    my_col = lax.axis_index("col")
    col_count = lax.axis_size("col")
    rhs_count = rhs.shape[0]
    slab_rows = factor.shape[0]
    rounds = factor.shape[1]
    piece_len = factor.shape[3]
    block_len = diag_inv.shape[1]
    pieces = block_len // piece_len
    blocks_here = slab_rows // block_len
    total_blocks = blocks_here * lax.axis_size("row")
    first_column = (my_row * col_count + my_col) * rhs.shape[1]
    source_len = rhs.shape[1]
    located = pivots - first_column
    inside = (located >= 0) & (located < source_len)
    taken = jnp.take(rhs, jnp.clip(located, 0, source_len - 1), axis=1)
    taken = jnp.where(inside[None, :], taken, 0.0)
    permuted = lax.psum_scatter(
        jnp.transpose(
            taken.reshape(rhs_count, blocks_here * lax.axis_size("row"), block_len), (1, 0, 2)
        ),
        "row",
        scatter_dimension=0,
        tiled=True,
    )
    permuted = lax.psum(permuted, "col")
    factor_rows = factor.reshape(slab_rows, rounds * piece_len)

    def advance(number, solved):
        owner_row = number // blocks_here
        local_block = number % blocks_here
        block_rows = lax.dynamic_slice_in_dim(factor_rows, local_block * block_len, block_len, 0)
        partial_value = lax.dot_general(
            solved.reshape(rhs_count, rounds * piece_len),
            block_rows,
            (((1,), (1,)), ((), ())),
            precision=lax.Precision.HIGHEST,
            preferred_element_type=jnp.float32,
        )
        own_rhs = lax.dynamic_index_in_dim(permuted, local_block, 0, keepdims=False)
        block_inv = lax.dynamic_index_in_dim(diag_inv, local_block, 0, keepdims=False)
        summed = lax.psum(partial_value, "col")
        fresh = apply_inverse(own_rhs - summed, block_inv)
        fresh = broadcast(fresh, "row", owner_row)
        first_piece = number * pieces
        offset_piece = (my_col - first_piece) % col_count
        owns = offset_piece < pieces
        which = jnp.clip(offset_piece, 0, pieces - 1)
        local_round = jnp.clip((first_piece + offset_piece) // col_count, 0, rounds - 1)
        piece = lax.dynamic_slice_in_dim(fresh, which * piece_len, piece_len, 1)
        updated = lax.dynamic_update_index_in_dim(solved, piece[:, None, :], local_round, 1)
        return jnp.where(owns, updated, solved)

    start_state = jnp.zeros((rhs_count, rounds, 1, piece_len), jnp.float32)
    return lax.fori_loop(0, total_blocks, advance, start_state)


MESH = pl.DeviceIdType.MESH
def split(a):
    hi = a.astype(jnp.bfloat16)
    return hi, (a - hi.astype(jnp.float32)).astype(jnp.bfloat16)


def dot3(a, b, transposed=False):
    dims = (((1,), (1 if transposed else 0,)), ((), ()))
    one = functools.partial(
        lax.dot_general, dimension_numbers=dims, preferred_element_type=jnp.float32
    )
    return one(a[0], b[0]) + (one(a[0], b[1]) + one(a[1], b[0]))


def solve_kernel(
    rows,
    cols,
    rhs_ref,
    piv_ref,
    fac_ref,
    diag_ref,
    out_ref,
    lf,
    dg,
    dh,
    dl,
    g,
    s0,
    a1,
    ab,
    zbuf,
    brow,
    l10,
    lh,
    ll,
    mh,
    ml,
    w,
    part,
    pbuf,
    ybuf,
    local_sem,
    ssend,
    srecv,
    zsend,
    zrecv,
    gsend,
    grecv,
    lsend,
    lrecv,
    psend,
    precv,
    ysend,
    yrecv,
):
    r = lax.axis_index("row")
    c = lax.axis_index("col")
    core, x, y = c % 2, (c // 2) % 2, c // 4
    nrhs, source_len = rhs_ref.shape
    blk = dg.shape[1]
    plen = lf.shape[2]
    slots = cols // 2
    to_core = c + 1 - 2 * core
    to_x = c + 2 * (1 - 2 * x)
    to_y = c + 4 * (1 - 2 * y)

    fetch = [
        pltpu.make_async_copy(fac_ref.at[:, k, 0, :], lf.at[k], local_sem.at[k])
        for k in range(rows)
    ]
    for copy in fetch:
        copy.start()
    fetch_d = pltpu.make_async_copy(diag_ref, dg, local_sem.at[rows])
    fetch_d.start()

    barrier = pltpu.get_barrier_semaphore()
    for d in range(1, cols):
        pl.semaphore_signal(barrier, inc=1, device_id=(r, (c + d) % cols), device_id_type=MESH)
    for d in range(1, rows):
        pl.semaphore_signal(barrier, inc=1, device_id=((r + d) % rows, c), device_id_type=MESH)

    def remote(src, dst, send, recv, row, col):
        return pltpu.make_async_remote_copy(
            src_ref=src,
            dst_ref=dst,
            send_sem=send,
            recv_sem=recv,
            device_id=(row, col),
            device_id_type=MESH,
        )

    first_tile = (r * cols + c) * (source_len // plen)

    def pick(p, side):
        @pl.loop(0, 4)
        def _(i):
            f, s = i // 2, i % 2
            q = (s * 4 + f * 2 if p % 2 == 0 else f * 4 + s * 2) + side + p * cols
            wanted = jnp.broadcast_to(piv_ref[q], (8, plen))
            lane = wanted % plen
            tile = wanted // plen - first_tile
            for n in range(nrhs // 8):
                found = jnp.zeros((8, plen), jnp.float32)
                for t in range(source_len // plen):
                    got = jnp.take_along_axis(
                        rhs_ref[n * 8 : n * 8 + 8, t * plen : (t + 1) * plen],
                        lane,
                        axis=1,
                        mode="promise_in_bounds",
                    )
                    found = jnp.where(tile == t, got, found)
                g[p, side, f, s, n * 8 : n * 8 + 8, :] = found

    mine = c % slots
    xflip = mine + 2 * (1 - 2 * x)
    ly = remote(l10.at[mine], l10.at[mine], lsend.at[0], lrecv.at[0], r, to_y)
    lx = remote(l10.at[mine], l10.at[mine], lsend.at[1], lrecv.at[1], r, to_x)
    lc = remote(l10.at[mine], l10.at[mine], lsend.at[2], lrecv.at[2], r, to_core)
    lb = remote(l10.at[xflip], l10.at[xflip], lsend.at[3], lrecv.at[3], r, to_core)

    c0, c1, c2, cz = [], [], [], []
    for p in range(rows):
        near, far = ((x, to_x), (y, to_y)) if p % 2 == 0 else ((y, to_y), (x, to_x))
        c0.append(
            remote(g.at[p, 1 - core], s0.at[p], ssend.at[p], srecv.at[p], r, to_core)
        )
        c1.append(
            remote(
                s0.at[p, 1 - near[0]],
                a1.at[p],
                ssend.at[rows + p],
                srecv.at[rows + p],
                r,
                near[1],
            )
        )
        c2.append(
            remote(
                a1.at[p, 1 - far[0]],
                ab.at[p],
                ssend.at[2 * rows + p],
                srecv.at[2 * rows + p],
                r,
                far[1],
            )
        )
        hop = (p - r + rows) % rows
        cz.append(remote(ab.at[p], zbuf.at[hop], zsend.at[p], zrecv.at[hop], p, c))
    gc = [
        remote(brow.at[c], brow.at[c], gsend.at[d], grecv.at[d], r, (c + d) % cols)
        for d in range(1, cols)
    ]

    def landed_core(p):
        c0[p].wait()
        s0[p] += g[p, core]
        c1[p].start()

    def landed_near(p):
        near, far = (x, y) if p % 2 == 0 else (y, x)
        c1[p].wait()
        a1[p] += s0[p, near]
        c2[p].start()

    def landed_far(p):
        far = y if p % 2 == 0 else x
        c2[p].wait()
        ab[p] += a1[p, far]

        @pl.when(r != p)
        def _():
            cz[p].start()

    def landed_row(p):
        @pl.when(r == p)
        def _():
            piece = ab[p]
            for d in range(1, rows):
                remote(
                    ab.at[p], zbuf.at[d], zsend.at[p], zrecv.at[d], (p + d) % rows, c
                ).wait_recv()
                piece = piece + zbuf[d]
            brow[c] = piece
            for copy in gc:
                copy.start()

    for step in range(rows + 4):
        if step < rows:
            pick(step, 1 - core)
            if step == 0:
                pl.semaphore_wait(barrier, cols + rows - 2)
            c0[step].start()
            pick(step, core)
        if step == 0:
            for copy in fetch:
                copy.wait()

            @pl.when(y == 0)
            def _():
                l10[mine] = lf[r, blk:, :]
                ly.start()

        for stage, act in ((4, landed_row), (3, landed_far), (2, landed_near), (1, landed_core)):
            if 0 <= step - stage < rows:
                act(step - stage)
        if step == 3:

            @pl.when(y == 1)
            def _():
                ly.wait_recv()

            lx.start()
            lc.start()

    fetch_d.wait()
    for i in range(2):
        dh[i], dl[i] = split(dg[i])

    def top(k, carry):
        th, tl = split(dot3((dh[0], dl[0]), split(lf[k, :blk, :])))
        mh[k, :blk, :] = th
        ml[k, :blk, :] = tl
        return carry

    lax.fori_loop(0, r, top, 0)

    lx.wait_recv()
    lb.start()
    lc.wait_recv()
    lb.wait_recv()
    for t in range(slots):
        lh[:, t * plen : (t + 1) * plen], ll[:, t * plen : (t + 1) * plen] = split(l10[t])

    rows_here = pl.ds(pl.multiple_of(mine * plen, plen), plen)

    @pl.when(c < slots)
    def _():
        w[:, :blk] = dg[0, rows_here, :]
        w[:, blk:] = jnp.zeros((plen, blk), jnp.float32)

    @pl.when(c >= slots)
    def _():
        w[:, blk:] = dg[1, rows_here, :]
        u = dot3((dh[1, rows_here, :], dl[1, rows_here, :]), (lh[...], ll[...]))
        w[:, :blk] = -dot3(split(u), (dh[0], dl[0]))

    def bottom(k, carry):
        low = lf[k, blk:, :] - dot3((lh[...], ll[...]), (mh[k, :blk, :], ml[k, :blk, :]))
        bh, bl = split(dot3((dh[1], dl[1]), split(low)))
        mh[k, blk:, :] = bh
        ml[k, blk:, :] = bl
        return carry

    lax.fori_loop(0, r, bottom, 0)

    for copy in gc:
        copy.wait_recv()
    b = jnp.concatenate([brow[s] for s in range(cols)], axis=1)
    own = dot3(split(b), split(w[...]), True)

    pc = [
        remote(
            part.at[(c + d) % cols], pbuf.at[d], psend.at[d], precv.at[d], r, (c + d) % cols
        )
        for d in range(1, cols)
    ]
    for k in range(rows):
        yc = [
            remote(ybuf.at[k], ybuf.at[k], ysend.at[d], yrecv.at[k], (k + d) % rows, c)
            for d in range(1, rows)
        ]

        @pl.when(r == k)
        def _():
            if k == 0:
                ybuf[k] = own
            else:
                total = part[c]
                for d in range(1, cols):
                    pc[d - 1].wait_recv()
                    total = total + pbuf[d]
                ybuf[k] = own - total
            for copy in yc:
                copy.start()

        @pl.when(r != k)
        def _():
            yc[0].wait_recv()

        if k < rows - 1:

            @pl.when(r > k)
            def _():
                add = dot3(split(ybuf[k]), (mh[k], ml[k]), True)
                for p in range(cols):
                    now = add[:, p * plen : (p + 1) * plen]
                    part[p] = now if k == 0 else part[p] + now

            @pl.when(r == k + 1)
            def _():
                for copy in pc:
                    copy.start()

    out_ref[...] = ybuf[...]

    for p in range(rows):

        @pl.when(r != p)
        def _():
            cz[p].wait_send()

    @pl.when(y == 0)
    def _():
        ly.wait_send()

    lx.wait_send()
    lc.wait_send()
    lb.wait_send()
    for copy in gc:
        copy.wait_send()

    @pl.when(r > 0)
    def _():
        for copy in pc:
            copy.wait_send()

    for d in range(1, rows):
        remote(
            ybuf.at[r], ybuf.at[r], ysend.at[d], yrecv.at[r], (r + d) % rows, c
        ).wait_send()


def per_device_fast(rows, cols, rhs, pivots, factor, diag_inv):
    nrhs = rhs.shape[0]
    plen = factor.shape[3]
    blk = diag_inv.shape[1]
    slab = factor.shape[0]
    slots = cols // 2
    f32, bf16 = jnp.float32, jnp.bfloat16
    dma = pltpu.SemaphoreType.DMA
    solved = pl.pallas_call(
        functools.partial(solve_kernel, rows, cols),
        out_shape=jax.ShapeDtypeStruct((rows, nrhs, plen), f32),
        in_specs=[
            pl.BlockSpec(memory_space=pltpu.VMEM),
            pl.BlockSpec(memory_space=pltpu.VMEM),
            pl.BlockSpec(memory_space=pl.ANY),
            pl.BlockSpec(memory_space=pl.ANY),
        ],
        out_specs=pl.BlockSpec(memory_space=pltpu.VMEM),
        scratch_shapes=[
            pltpu.VMEM((rows, slab, plen), f32),
            pltpu.VMEM((2, blk, blk), f32),
            pltpu.VMEM((2, blk, blk), bf16),
            pltpu.VMEM((2, blk, blk), bf16),
            pltpu.VMEM((rows, 2, 2, 2, nrhs, plen), f32),
            pltpu.VMEM((rows, 2, 2, nrhs, plen), f32),
            pltpu.VMEM((rows, 2, nrhs, plen), f32),
            pltpu.VMEM((rows, nrhs, plen), f32),
            pltpu.VMEM((rows, nrhs, plen), f32),
            pltpu.VMEM((cols, nrhs, plen), f32),
            pltpu.VMEM((slots, blk, plen), f32),
            pltpu.VMEM((blk, blk), bf16),
            pltpu.VMEM((blk, blk), bf16),
            pltpu.VMEM((rows - 1, slab, plen), bf16),
            pltpu.VMEM((rows - 1, slab, plen), bf16),
            pltpu.VMEM((plen, slab), f32),
            pltpu.VMEM((cols, nrhs, plen), f32),
            pltpu.VMEM((cols, nrhs, plen), f32),
            pltpu.VMEM((rows, nrhs, plen), f32),
            dma((rows + 1,)),
            dma((3 * rows,)),
            dma((3 * rows,)),
            dma((rows,)),
            dma((rows,)),
            dma((cols,)),
            dma((cols,)),
            dma((4,)),
            dma((4,)),
            dma((cols,)),
            dma((cols,)),
            dma((rows,)),
            dma((rows,)),
        ],
        compiler_params=pltpu.CompilerParams(collective_id=0, has_side_effects=True),
    )(rhs, pivots.reshape(rows * cols, 1, plen), factor, diag_inv)
    return jnp.transpose(solved, (1, 0, 2))[:, :, None, :]


def per_device(rhs, pivots, factor, diag_inv):
    rows = lax.axis_size("row")
    cols = lax.axis_size("col")
    slab, rounds, _, plen = factor.shape
    blk = diag_inv.shape[1]
    if cols == 8 and slab == 2 * blk == cols * plen and rounds == rows and rhs.shape[1] % plen == 0:
        return per_device_fast(rows, cols, rhs, pivots, factor, diag_inv)
    return per_device_general(rhs, pivots, factor, diag_inv)


def solution(mesh):
    return jax.shard_map(
        per_device,
        mesh=mesh,
        in_specs=(P(None, ("row", "col")), P(), P("row", None, "col", None), P("row", None, None)),
        out_specs=P(None, None, "col", None),
        check_vma=False,
    )
```

```python
import functools

import jax
import jax.numpy as jnp
from jax import lax
from jax.experimental import pallas as pl
from jax.experimental.pallas import tpu as pltpu
from jax.sharding import PartitionSpec as P


def broadcast(shard, axis, root):
    mine = lax.axis_index(axis) == root
    return lax.psum(jnp.where(mine, shard, jnp.zeros_like(shard)), axis)


def apply_inverse(values, block_inv):
    return lax.dot_general(
        values,
        block_inv,
        (((1,), (1,)), ((), ())),
        precision=lax.Precision.HIGHEST,
        preferred_element_type=jnp.float32,
    )


def per_device_general(rhs, pivots, factor, diag_inv):
    my_row = lax.axis_index("row")
    my_col = lax.axis_index("col")
    col_count = lax.axis_size("col")
    rhs_count = rhs.shape[0]
    slab_rows = factor.shape[0]
    rounds = factor.shape[1]
    piece_len = factor.shape[3]
    block_len = diag_inv.shape[1]
    pieces = block_len // piece_len
    blocks_here = slab_rows // block_len
    total_blocks = blocks_here * lax.axis_size("row")
    first_column = (my_row * col_count + my_col) * rhs.shape[1]
    source_len = rhs.shape[1]
    located = pivots - first_column
    inside = (located >= 0) & (located < source_len)
    taken = jnp.take(rhs, jnp.clip(located, 0, source_len - 1), axis=1)
    taken = jnp.where(inside[None, :], taken, 0.0)
    permuted = lax.psum_scatter(
        jnp.transpose(
            taken.reshape(rhs_count, blocks_here * lax.axis_size("row"), block_len), (1, 0, 2)
        ),
        "row",
        scatter_dimension=0,
        tiled=True,
    )
    permuted = lax.psum(permuted, "col")
    factor_rows = factor.reshape(slab_rows, rounds * piece_len)

    def advance(number, solved):
        owner_row = number // blocks_here
        local_block = number % blocks_here
        block_rows = lax.dynamic_slice_in_dim(factor_rows, local_block * block_len, block_len, 0)
        partial_value = lax.dot_general(
            solved.reshape(rhs_count, rounds * piece_len),
            block_rows,
            (((1,), (1,)), ((), ())),
            precision=lax.Precision.HIGHEST,
            preferred_element_type=jnp.float32,
        )
        own_rhs = lax.dynamic_index_in_dim(permuted, local_block, 0, keepdims=False)
        block_inv = lax.dynamic_index_in_dim(diag_inv, local_block, 0, keepdims=False)
        summed = lax.psum(partial_value, "col")
        fresh = apply_inverse(own_rhs - summed, block_inv)
        fresh = broadcast(fresh, "row", owner_row)
        first_piece = number * pieces
        offset_piece = (my_col - first_piece) % col_count
        owns = offset_piece < pieces
        which = jnp.clip(offset_piece, 0, pieces - 1)
        local_round = jnp.clip((first_piece + offset_piece) // col_count, 0, rounds - 1)
        piece = lax.dynamic_slice_in_dim(fresh, which * piece_len, piece_len, 1)
        updated = lax.dynamic_update_index_in_dim(solved, piece[:, None, :], local_round, 1)
        return jnp.where(owns, updated, solved)

    start_state = jnp.zeros((rhs_count, rounds, 1, piece_len), jnp.float32)
    return lax.fori_loop(0, total_blocks, advance, start_state)


MESH = pl.DeviceIdType.MESH
def split(a):
    hi = a.astype(jnp.bfloat16)
    return hi, (a - hi.astype(jnp.float32)).astype(jnp.bfloat16)


def dot3(a, b, transposed=False):
    dims = (((1,), (1 if transposed else 0,)), ((), ()))
    one = functools.partial(
        lax.dot_general, dimension_numbers=dims, preferred_element_type=jnp.float32
    )
    return one(a[0], b[0]) + (one(a[0], b[1]) + one(a[1], b[0]))


def solve_kernel(
    rows,
    cols,
    rhs_ref,
    piv_ref,
    fac_ref,
    diag_ref,
    out_ref,
    lf,
    dg,
    dh,
    dl,
    g,
    s0,
    a1,
    ab,
    zbuf,
    brow,
    l10,
    lh,
    ll,
    mh,
    ml,
    w,
    part,
    pbuf,
    ybuf,
    local_sem,
    ssend,
    srecv,
    zsend,
    zrecv,
    gsend,
    grecv,
    lsend,
    lrecv,
    psend,
    precv,
    ysend,
    yrecv,
):
    r = lax.axis_index("row")
    c = lax.axis_index("col")
    core, x, y = c % 2, (c // 2) % 2, c // 4
    nrhs, source_len = rhs_ref.shape
    blk = dg.shape[1]
    plen = lf.shape[2]
    slots = cols // 2
    to_core = c + 1 - 2 * core
    to_x = c + 2 * (1 - 2 * x)
    to_y = c + 4 * (1 - 2 * y)

    fetch = [
        pltpu.make_async_copy(fac_ref.at[:, k, 0, :], lf.at[k], local_sem.at[k])
        for k in range(rows)
    ]
    for copy in fetch:
        copy.start()
    fetch_d = pltpu.make_async_copy(diag_ref, dg, local_sem.at[rows])
    fetch_d.start()

    barrier = pltpu.get_barrier_semaphore()
    for d in range(1, cols):
        pl.semaphore_signal(barrier, inc=1, device_id=(r, (c + d) % cols), device_id_type=MESH)
    for d in range(1, rows):
        pl.semaphore_signal(barrier, inc=1, device_id=((r + d) % rows, c), device_id_type=MESH)

    def remote(src, dst, send, recv, row, col):
        return pltpu.make_async_remote_copy(
            src_ref=src,
            dst_ref=dst,
            send_sem=send,
            recv_sem=recv,
            device_id=(row, col),
            device_id_type=MESH,
        )

    first_tile = (r * cols + c) * (source_len // plen)

    def pick(p, side):
        @pl.loop(0, 4)
        def _(i):
            f, s = i // 2, i % 2
            q = (s * 4 + f * 2 if p % 2 == 0 else f * 4 + s * 2) + side + p * cols
            wanted = jnp.broadcast_to(piv_ref[q], (8, plen))
            lane = wanted % plen
            tile = wanted // plen - first_tile
            for n in range(nrhs // 8):
                found = jnp.zeros((8, plen), jnp.float32)
                for t in range(source_len // plen):
                    got = jnp.take_along_axis(
                        rhs_ref[n * 8 : n * 8 + 8, t * plen : (t + 1) * plen],
                        lane,
                        axis=1,
                        mode="promise_in_bounds",
                    )
                    found = jnp.where(tile == t, got, found)
                g[p, side, f, s, n * 8 : n * 8 + 8, :] = found

    mine = c % slots
    xflip = mine + 2 * (1 - 2 * x)
    ly = remote(l10.at[mine], l10.at[mine], lsend.at[0], lrecv.at[0], r, to_y)
    lx = remote(l10.at[mine], l10.at[mine], lsend.at[1], lrecv.at[1], r, to_x)
    lc = remote(l10.at[mine], l10.at[mine], lsend.at[2], lrecv.at[2], r, to_core)
    lb = remote(l10.at[xflip], l10.at[xflip], lsend.at[3], lrecv.at[3], r, to_core)

    c0, c1, c2, cz = [], [], [], []
    for p in range(rows):
        near, far = ((x, to_x), (y, to_y)) if p % 2 == 0 else ((y, to_y), (x, to_x))
        c0.append(
            remote(g.at[p, 1 - core], s0.at[p], ssend.at[p], srecv.at[p], r, to_core)
        )
        c1.append(
            remote(
                s0.at[p, 1 - near[0]],
                a1.at[p],
                ssend.at[rows + p],
                srecv.at[rows + p],
                r,
                near[1],
            )
        )
        c2.append(
            remote(
                a1.at[p, 1 - far[0]],
                ab.at[p],
                ssend.at[2 * rows + p],
                srecv.at[2 * rows + p],
                r,
                far[1],
            )
        )
        hop = (p - r + rows) % rows
        cz.append(remote(ab.at[p], zbuf.at[hop], zsend.at[p], zrecv.at[hop], p, c))
    gc = [
        remote(brow.at[c], brow.at[c], gsend.at[d], grecv.at[d], r, (c + d) % cols)
        for d in range(1, cols)
    ]

    def landed_core(p):
        c0[p].wait()
        s0[p] += g[p, core]
        c1[p].start()

    def landed_near(p):
        near, far = (x, y) if p % 2 == 0 else (y, x)
        c1[p].wait()
        a1[p] += s0[p, near]
        c2[p].start()

    def landed_far(p):
        far = y if p % 2 == 0 else x
        c2[p].wait()
        ab[p] += a1[p, far]

        @pl.when(r != p)
        def _():
            cz[p].start()

    def landed_row(p):
        @pl.when(r == p)
        def _():
            piece = ab[p]
            for d in range(1, rows):
                remote(
                    ab.at[p], zbuf.at[d], zsend.at[p], zrecv.at[d], (p + d) % rows, c
                ).wait_recv()
                piece = piece + zbuf[d]
            brow[c] = piece
            for copy in gc:
                copy.start()

    for step in range(rows + 4):
        if step < rows:
            pick(step, 1 - core)
            if step == 0:
                pl.semaphore_wait(barrier, cols + rows - 2)
            c0[step].start()
            pick(step, core)
        if step == 0:
            for copy in fetch:
                copy.wait()

            @pl.when(y == 0)
            def _():
                l10[mine] = lf[r, blk:, :]
                ly.start()

        for stage, act in ((4, landed_row), (3, landed_far), (2, landed_near), (1, landed_core)):
            if 0 <= step - stage < rows:
                act(step - stage)
        if step == 3:

            @pl.when(y == 1)
            def _():
                ly.wait_recv()

            lx.start()
            lc.start()

    fetch_d.wait()
    for i in range(2):
        dh[i], dl[i] = split(dg[i])

    def top(k, carry):
        th, tl = split(dot3((dh[0], dl[0]), split(lf[k, :blk, :])))
        mh[k, :blk, :] = th
        ml[k, :blk, :] = tl
        return carry

    lax.fori_loop(0, r, top, 0)

    lx.wait_recv()
    lb.start()
    lc.wait_recv()
    lb.wait_recv()
    for t in range(slots):
        lh[:, t * plen : (t + 1) * plen], ll[:, t * plen : (t + 1) * plen] = split(l10[t])

    rows_here = pl.ds(pl.multiple_of(mine * plen, plen), plen)

    @pl.when(c < slots)
    def _():
        w[:, :blk] = dg[0, rows_here, :]
        w[:, blk:] = jnp.zeros((plen, blk), jnp.float32)

    @pl.when(c >= slots)
    def _():
        w[:, blk:] = dg[1, rows_here, :]
        u = dot3((dh[1, rows_here, :], dl[1, rows_here, :]), (lh[...], ll[...]))
        w[:, :blk] = -dot3(split(u), (dh[0], dl[0]))

    def bottom(k, carry):
        low = lf[k, blk:, :] - dot3((lh[...], ll[...]), (mh[k, :blk, :], ml[k, :blk, :]))
        bh, bl = split(dot3((dh[1], dl[1]), split(low)))
        mh[k, blk:, :] = bh
        ml[k, blk:, :] = bl
        return carry

    lax.fori_loop(0, r, bottom, 0)

    for copy in gc:
        copy.wait_recv()
    b = jnp.concatenate([brow[s] for s in range(cols)], axis=1)
    own = dot3(split(b), split(w[...]), True)

    def pieces_of(h):
        return [
            remote(
                part.at[h, (c + d) % cols],
                pbuf.at[h, d],
                psend.at[h, d],
                precv.at[h, d],
                r,
                (c + d) % cols,
            )
            for d in range(1, cols)
        ]

    def news_of(k, h):
        return [
            remote(
                ybuf.at[k, h],
                ybuf.at[k, h],
                ysend.at[h, d],
                yrecv.at[h, k],
                (k + d) % rows,
                c,
            )
            for d in range(1, rows)
        ]

    chains = ybuf.shape[1]
    group = nrhs // chains
    for k in range(rows):
        for h in range(chains):
            pc = pieces_of(h)
            yc = news_of(k, h)
            own_h = own[h * group : (h + 1) * group]

            @pl.when(r == k)
            def _():
                if k == 0:
                    ybuf[k, h] = own_h
                else:
                    total = part[h, c]
                    for d in range(1, cols):
                        pc[d - 1].wait_recv()
                        total = total + pbuf[h, d]
                    ybuf[k, h] = own_h - total
                for copy in yc:
                    copy.start()

            @pl.when(r != k)
            def _():
                yc[0].wait_recv()

            if k < rows - 1:

                @pl.when(r > k)
                def _():
                    add = dot3(split(ybuf[k, h]), (mh[k], ml[k]), True)
                    for p in range(cols):
                        now = add[:, p * plen : (p + 1) * plen]
                        part[h, p] = now if k == 0 else part[h, p] + now

                @pl.when(r == k + 1)
                def _():
                    for copy in pc:
                        copy.start()

    for h in range(chains):
        out_ref[:, h * group : (h + 1) * group, :] = ybuf[:, h]

    @pl.when(r > 0)
    def _():
        for h in range(chains):
            for copy in pieces_of(h):
                copy.wait_send()

    for h in range(chains):
        for d in range(1, rows):
            remote(
                ybuf.at[r, h],
                ybuf.at[r, h],
                ysend.at[h, d],
                yrecv.at[h, r],
                (r + d) % rows,
                c,
            ).wait_send()

    for p in range(rows):

        @pl.when(r != p)
        def _():
            cz[p].wait_send()

    @pl.when(y == 0)
    def _():
        ly.wait_send()

    lx.wait_send()
    lc.wait_send()
    lb.wait_send()
    for copy in gc:
        copy.wait_send()


def per_device_fast(rows, cols, rhs, pivots, factor, diag_inv):
    nrhs = rhs.shape[0]
    plen = factor.shape[3]
    blk = diag_inv.shape[1]
    slab = factor.shape[0]
    slots = cols // 2
    chains = 2 if nrhs % 16 == 0 else 1
    f32, bf16 = jnp.float32, jnp.bfloat16
    dma = pltpu.SemaphoreType.DMA
    solved = pl.pallas_call(
        functools.partial(solve_kernel, rows, cols),
        out_shape=jax.ShapeDtypeStruct((rows, nrhs, plen), f32),
        in_specs=[
            pl.BlockSpec(memory_space=pltpu.VMEM),
            pl.BlockSpec(memory_space=pltpu.VMEM),
            pl.BlockSpec(memory_space=pl.ANY),
            pl.BlockSpec(memory_space=pl.ANY),
        ],
        out_specs=pl.BlockSpec(memory_space=pltpu.VMEM),
        scratch_shapes=[
            pltpu.VMEM((rows, slab, plen), f32),
            pltpu.VMEM((2, blk, blk), f32),
            pltpu.VMEM((2, blk, blk), bf16),
            pltpu.VMEM((2, blk, blk), bf16),
            pltpu.VMEM((rows, 2, 2, 2, nrhs, plen), f32),
            pltpu.VMEM((rows, 2, 2, nrhs, plen), f32),
            pltpu.VMEM((rows, 2, nrhs, plen), f32),
            pltpu.VMEM((rows, nrhs, plen), f32),
            pltpu.VMEM((rows, nrhs, plen), f32),
            pltpu.VMEM((cols, nrhs, plen), f32),
            pltpu.VMEM((slots, blk, plen), f32),
            pltpu.VMEM((blk, blk), bf16),
            pltpu.VMEM((blk, blk), bf16),
            pltpu.VMEM((rows - 1, slab, plen), bf16),
            pltpu.VMEM((rows - 1, slab, plen), bf16),
            pltpu.VMEM((plen, slab), f32),
            pltpu.VMEM((chains, cols, nrhs // chains, plen), f32),
            pltpu.VMEM((chains, cols, nrhs // chains, plen), f32),
            pltpu.VMEM((rows, chains, nrhs // chains, plen), f32),
            dma((rows + 1,)),
            dma((3 * rows,)),
            dma((3 * rows,)),
            dma((rows,)),
            dma((rows,)),
            dma((cols,)),
            dma((cols,)),
            dma((4,)),
            dma((4,)),
            dma((chains, cols)),
            dma((chains, cols)),
            dma((chains, rows)),
            dma((chains, rows)),
        ],
        compiler_params=pltpu.CompilerParams(collective_id=0, has_side_effects=True),
    )(rhs, pivots.reshape(rows * cols, 1, plen), factor, diag_inv)
    return jnp.transpose(solved, (1, 0, 2))[:, :, None, :]


def per_device(rhs, pivots, factor, diag_inv):
    rows = lax.axis_size("row")
    cols = lax.axis_size("col")
    slab, rounds, _, plen = factor.shape
    blk = diag_inv.shape[1]
    if cols == 8 and slab == 2 * blk == cols * plen and rounds == rows and rhs.shape[1] % plen == 0:
        return per_device_fast(rows, cols, rhs, pivots, factor, diag_inv)
    return per_device_general(rhs, pivots, factor, diag_inv)


def solution(mesh):
    return jax.shard_map(
        per_device,
        mesh=mesh,
        in_specs=(P(None, ("row", "col")), P(), P("row", None, "col", None), P("row", None, None)),
        out_specs=P(None, None, "col", None),
        check_vma=False,
    )
```
